16 devices in a mesh: dp: 4 (over y, z, core), tp: 4 (over x).
Axes of the slice: x: 4, y: 2, z: 1, core: 2. Of those that a mesh axis runs over, the one named last changes fastest.
The devices are a block of a 4x4x4 slice.
Arguments:
- x: bfloat16 [2560, 6656], P(('dp', 'tp')), parts along dimension 0
- dy: bfloat16 [2560, 6656], P(('dp', 'tp')), parts along dimension 0
- gate: bfloat16 [2560, 17920], P('dp', 'tp'), parts along dimension 0
- up: bfloat16 [2560, 17920], P('dp', 'tp'), parts along dimension 0
- w_gate: bfloat16 [6656, 17920], P(None, 'tp')
- w_up: bfloat16 [6656, 17920], P(None, 'tp')
- w_down: bfloat16 [17920, 6656], P('tp')
Outputs:
- output 1: bfloat16 [2560, 6656], P(('dp', 'tp')), parts along dimension 0
- output 2: bfloat16 [26624, 17920], P('dp', 'tp'), parts along dimension 0
- output 3: bfloat16 [26624, 17920], P('dp', 'tp'), parts along dimension 0
- output 4: bfloat16 [71680, 6656], P(('dp', 'tp')), parts along dimension 0
There are 4 independent parts. The reference program is written for one: setup_inputs(seed, part) draws one part's arguments, and reference() takes and returns one part's arrays. A program takes and returns all parts, laid end to end along the dimension named above; an argument that names none is the same for every part.
All inputs are finite; a program needn't handle non-finite values.
Results may differ from the reference program's by a relative error of at most 0.012.
Values are sent between devices in bfloat16 or wider.
A program may use at most 1.5 GiB of HBM per device.

```python
import jax
import jax.numpy as jnp

ROWS = 640
D = 6656
FF = 17920


def act(gate, up):
    return jax.nn.silu(gate) * up


def setup_inputs(seed: int = 0, part: int = 0) -> dict:
    kx, ky, ka, kb, kg, ku, kd = jax.random.split(jax.random.key(seed), 7)
    kx, ky, ka, kb = (jax.random.fold_in(k, part) for k in (kx, ky, ka, kb))
    drawn = {
        "x": jax.random.normal(kx, (ROWS, D), jnp.float32),
        "dy": jax.random.normal(ky, (ROWS, D), jnp.float32),
        "gate": jax.random.normal(ka, (ROWS, FF), jnp.float32),
        "up": jax.random.normal(kb, (ROWS, FF), jnp.float32),
        "w_gate": jax.random.normal(kg, (D, FF), jnp.float32) * D**-0.5,
        "w_up": jax.random.normal(ku, (D, FF), jnp.float32) * D**-0.5,
        "w_down": jax.random.normal(kd, (FF, D), jnp.float32) * FF**-0.5,
    }
    return {k: v.astype(jnp.bfloat16) for k, v in drawn.items()}


def reference(x, dy, gate, up, w_gate, w_up, w_down):
    hidden, back = jax.vjp(act, gate.astype(jnp.float32), up.astype(jnp.float32))
    d_hidden = jnp.dot(dy, w_down.T, preferred_element_type=jnp.float32)
    d_gate, d_up = (g.astype(jnp.bfloat16) for g in back(d_hidden))
    dx = jnp.dot(d_gate, w_gate.T, preferred_element_type=jnp.float32) + jnp.dot(d_up, w_up.T, preferred_element_type=jnp.float32)
    dw_gate = jnp.dot(x.T, d_gate, preferred_element_type=jnp.float32)
    dw_up = jnp.dot(x.T, d_up, preferred_element_type=jnp.float32)
    dw_down = jnp.dot(hidden.astype(jnp.bfloat16).T, dy, preferred_element_type=jnp.float32)
    return tuple(g.astype(jnp.bfloat16) for g in (dx, dw_gate, dw_up, dw_down))
```

```python
import functools

import jax
import jax.numpy as jnp
from jax import lax
from jax.experimental import pallas as pl
from jax.experimental.pallas import tpu as pltpu
from jax.sharding import PartitionSpec as P

MESH = pl.DeviceIdType.MESH
BF16, F32 = jnp.bfloat16, jnp.float32
BLK = 512
LATE = 3
ROWS = 16
VMEM_LIMIT = 66_500_000

NT = (((1,), (1,)), ((), ()))
NN = (((1,), (0,)), ((), ()))


def dot(a, b, dims):
    return lax.dot_general(a, b, dims, preferred_element_type=F32)


def act_parts(gate, up):
    g, u = gate.astype(F32), up.astype(F32)
    s = 1.0 / (1.0 + jnp.exp(-g))
    return g, u, s


def fused_kernel(
    n, x_own, dy_own, gate, up, wg, wu, wd,
    dwd, dcat_out, dxp, xg,
    dyg, dcat, acc, hid, wb, gu,
    d_send, d_recv, d_own, x_send, x_recv, x_in, x_out, w_sem, w_last, o_sem, l_sem, gu_sem, dx_sem, dc_sem,
):
    own, depth = dy_own.shape
    rows, ff = gate.shape
    nb = depth // BLK
    nf, rem = ff // BLK, ff % BLK
    half = own // 2
    side = BLK - rem
    tail = rem - side
    np1 = nf + 1
    me = lax.axis_index("tp")
    right, left = lax.rem(me + 1, n), lax.rem(me + n - 1, n)

    def cols(b):
        return pl.ds(pl.multiple_of(b * BLK, BLK), BLK)

    def own_rows(i):
        return pl.ds(pl.multiple_of(i * own, 16), own)

    def half_rows(i, second):
        return pl.ds(pl.multiple_of(i * own + second * half, 16), half)

    def remote(src, dst, send, recv, to):
        return pltpu.make_async_remote_copy(
            src_ref=src, dst_ref=dst, send_sem=send, recv_sem=recv, device_id={"tp": to}, device_id_type=MESH
        )

    def view(which, b, r):
        return dyg.at[b, r] if which == "d" else xg.at[r, cols(b)]

    def sems(which):
        return (d_send, d_recv) if which == "d" else (x_send, x_recv)

    def hop_copy(which, b, i):
        src = (dy_own if which == "d" else x_own).at[:, cols(b)]
        send, recv = sems(which)
        return remote(src, view(which, b, own_rows(me)), send.at[b, i], recv.at[b, i], (right, left)[i])

    def fwd_copy(which, b, i):
        r = half_rows((left, right)[i], i)
        send, recv = sems(which)
        return remote(view(which, b, r), view(which, b, r), send.at[b, 2 + i], recv.at[b, 2 + i], (right, left)[i])

    def hop(which, b):
        for i in (0, 1):
            hop_copy(which, b, i).start()

    def fwd(which, b):
        for i in (0, 1):
            r = own_rows((left, right)[i])
            send, recv = sems(which)
            remote(view(which, b, r), view(which, b, r), send.at[b, i], recv.at[b, i], right).wait_recv()
            fwd_copy(which, b, i).start()

    def far(which, b):
        opposite = lax.rem(me + 2, n)
        send, recv = sems(which)
        for i in (0, 1):
            r = half_rows(opposite, i)
            remote(view(which, b, r), view(which, b, r), send.at[b, 2 + i], recv.at[b, 2 + i], right).wait_recv()

    def sent(which, b):
        for i in (0, 1):
            hop_copy(which, b, i).wait_send()
            fwd_copy(which, b, i).wait_send()

    def own_copy(b):
        return pltpu.make_async_copy(dy_own.at[:, cols(b)], dyg.at[b, own_rows(me)], d_own.at[b])

    def size(p):
        return BLK if p < nf else rem

    def wd_copies(b, s):
        return [
            pltpu.make_async_copy(
                wd.at[pl.ds(p * BLK, size(p)), cols(b)], wb.at[s, p, pl.ds(0, size(p))], w_sem.at[s, p]
            )
            for p in range(np1)
        ]

    def out_copies(b, s):
        return [
            pltpu.make_async_copy(
                wb.at[s, np1 + p, pl.ds(0, size(p))], dwd.at[pl.ds(p * BLK, size(p)), cols(b)], o_sem.at[s, p]
            )
            for p in range(np1)
        ]

    def wx_copies(b, s):
        r = cols(b)
        c = [
            pltpu.make_async_copy((wg, wu)[i].at[r, pl.ds(p * BLK, BLK)], wb.at[s, i * nf + p], w_sem.at[s, i * nf + p])
            for i in (0, 1)
            for p in range(nf)
        ]
        e = nf * BLK
        c.append(
            pltpu.make_async_copy(wg.at[r, pl.ds(e, rem)], wb.at[s, 2 * nf, :, pl.ds(0, rem)], w_sem.at[s, 2 * nf])
        )
        c.append(
            pltpu.make_async_copy(wu.at[r, pl.ds(e, side)], wb.at[s, 2 * nf, :, pl.ds(rem, side)], w_last.at[s])
        )
        c.append(
            pltpu.make_async_copy(
                wu.at[r, pl.ds(e + side, tail)], wb.at[s, 2 * nf + 1, :, pl.ds(0, tail)], w_sem.at[s, 2 * nf + 1]
            )
        )
        return c

    def gu_copies(p, s, width):
        c = pl.ds(pl.multiple_of(p * BLK, BLK), width)
        return [
            pltpu.make_async_copy((gate, up)[i].at[:, c], gu.at[2 * s + i, :, pl.ds(0, width)], gu_sem.at[s, i])
            for i in (0, 1)
        ]

    def late_copies(p, q, width):
        r = pl.ds(pl.multiple_of(p * BLK, BLK), width)
        return [
            pltpu.make_async_copy(
                wb.at[1, np1 + LATE * q + k, pl.ds(0, width)], dwd.at[r, cols(nb - LATE + k)], l_sem.at[q, k]
            )
            for k in range(LATE)
        ]

    def start(copies):
        for c in copies:
            c.start()

    def wait(copies):
        for c in copies:
            c.wait()

    barrier = pltpu.get_barrier_semaphore()
    for to in (left, right):
        pl.semaphore_signal(barrier, inc=1, device_id={"tp": to}, device_id_type=MESH)
    start(gu_copies(0, 0, BLK))
    start(gu_copies(1, 1, BLK))
    pl.semaphore_wait(barrier, 2)
    for b in range(3):
        hop("d", b)
    for b in range(nb):
        own_copy(b).start()
    start(wd_copies(0, 0))
    start(wd_copies(1, 1))

    def hidden_piece(p, s, width):
        wait(gu_copies(p, s, width))
        for r in range(0, rows, 128):
            for c in range(0, width, 128):
                g, u, sg = act_parts(gu[2 * s, r : r + 128, c : c + 128], gu[2 * s + 1, r : r + 128, c : c + 128])
                hid[p, c : c + 128, r : r + 128] = (g * sg * u).astype(BF16).T
        acc[p, :, :width] = jnp.zeros((rows, width), F32)

    def hidden_full(p, _):
        s = lax.rem(p, 2)
        hidden_piece(p, s, BLK)

        @pl.when(p < nf - 2)
        def _():
            start(gu_copies(p + 2, s, BLK))

        @pl.when(p == nf - 2)
        def _():
            start(gu_copies(nf, s, rem))

        return 0

    lax.fori_loop(0, nf // 2, hidden_full, 0)
    fwd("d", 0)
    hop("d", 3)
    lax.fori_loop(nf // 2, nf, hidden_full, 0)
    hidden_piece(nf, nf % 2, rem)
    fwd("d", 1)
    hop("d", 4)

    def d_hidden(b, s):
        dyb = dyg[b]
        for p in range(np1):
            w = size(p)
            acc[p, :, :w] += dot(dyb, wb[s, p, :w, :], NT)

    def both(b, _):
        s = lax.rem(b, 2)
        fwd("d", b + 2)

        @pl.when(b < nb - 5)
        def _():
            hop("d", b + 5)

        wait(wd_copies(b, s))
        own_copy(b).wait()
        far("d", b)

        @pl.when(b >= 2)
        def _():
            wait(out_copies(b - 2, s))

        d_hidden(b, s)
        dyb = dyg[b]
        for p in range(np1):
            w = size(p)
            wb[s, np1 + p, :w, :] = dot(hid[p, :w, :], dyb, NN).astype(BF16)
        start(out_copies(b, s))
        start(wd_copies(b + 2, s))
        return 0

    lax.fori_loop(0, nb - LATE, both, 0)

    start(gu_copies(0, 0, BLK))
    start(gu_copies(1, 1, BLK))

    def only_hidden(b, _):
        s = lax.rem(b, 2)

        @pl.when(b == nb - 3)
        def _():
            fwd("d", nb - 1)

        wait(wd_copies(b, s))
        own_copy(b).wait()
        far("d", b)
        d_hidden(b, s)

        @pl.when(b == nb - 3)
        def _():
            start(wd_copies(nb - 1, s))

        return 0

    lax.fori_loop(nb - LATE, nb, only_hidden, 0)
    for b in (nb - LATE - 2, nb - LATE - 1):
        wait(out_copies(b, b % 2))
    start(wx_copies(0, 0))
    for b in range(3):
        hop("x", b)

    def act_piece(p, s, width, first):
        wait(gu_copies(p, s, width))
        if first is None:
            wait(late_copies(p - 2, s, BLK))
        else:

            @pl.when(first)
            def _():
                wait(late_copies(p - 2, s, BLK))

        for r in range(0, rows, ROWS):
            t = slice(r, r + ROWS)
            g, u, sg = act_parts(gu[2 * s, t, :width], gu[2 * s + 1, t, :width])
            dh = acc[p, t, :width]
            silu = g * sg
            d_up = (dh * silu).astype(BF16)
            d_gate = (dh * u * (sg + silu * (1.0 - sg))).astype(BF16)
            if width == BLK:
                dcat[p, t, :] = d_gate
                dcat[nf + p, t, :] = d_up
            else:
                dcat[2 * nf, t, :rem] = d_gate
                dcat[2 * nf, t, rem:] = d_up[:, :side]
                dcat[2 * nf + 1, t, :tail] = d_up[:, side:]
        for k in range(LATE):
            wb[1, np1 + LATE * s + k, :width, :] = dot(hid[p, :width, :], dyg[nb - LATE + k], NN).astype(BF16)
        start(late_copies(p, s, width))

    def act_full(p, _):
        s = lax.rem(p, 2)
        act_piece(p, s, BLK, p >= 2)

        @pl.when(p < nf - 2)
        def _():
            start(gu_copies(p + 2, s, BLK))

        @pl.when(p == nf - 2)
        def _():
            start(gu_copies(nf, s, rem))

        return 0

    lax.fori_loop(0, nf, act_full, 0)
    act_piece(nf, nf % 2, rem, None)
    wait(late_copies(nf - 1, (nf - 1) % 2, BLK))
    wait(late_copies(nf, nf % 2, rem))
    start(wx_copies(1, 1))

    def dcat_copies():
        c = [pltpu.make_async_copy(dcat.at[p], dcat_out.at[p], dc_sem.at[p]) for p in range(2 * nf + 1)]
        c.append(
            pltpu.make_async_copy(
                dcat.at[2 * nf + 1, :, pl.ds(0, tail)], dcat_out.at[2 * nf + 1, :, pl.ds(0, tail)], dc_sem.at[2 * nf + 1]
            )
        )
        return c

    start(dcat_copies())

    def dx_copy(b, s):
        return pltpu.make_async_copy(gu.at[s], dxp.at[:, cols(b)], dx_sem.at[s])

    def x_in_copy(b, s):
        return pltpu.make_async_copy(x_own.at[:, cols(b)], gu.at[2 + s, pl.ds(0, own)], x_in.at[s])

    def x_out_copy(b, s):
        return pltpu.make_async_copy(gu.at[2 + s, pl.ds(0, own)], xg.at[own_rows(me), cols(b)], x_out.at[s])

    x_in_copy(0, 0).start()

    def dx_block(b, _):
        s = lax.rem(b, 2)
        fwd("x", b)

        @pl.when(b < nb - 3)
        def _():
            hop("x", b + 3)

        x_in_copy(b, s).wait()
        x_out_copy(b, s).start()

        @pl.when(b >= 1)
        def _():
            x_out_copy(b - 1, 1 - s).wait()

        @pl.when(b < nb - 1)
        def _():
            x_in_copy(b + 1, 1 - s).start()

        @pl.when(b >= 2)
        def _():
            dx_copy(b - 2, s).wait()

        wait(wx_copies(b, s))
        total = dot(dcat[0], wb[s, 0], NT)
        for p in range(1, 2 * nf + 1):
            total += dot(dcat[p], wb[s, p], NT)
        total += dot(dcat[2 * nf + 1, :, :tail], wb[s, 2 * nf + 1, :, :tail], NT)
        gu[s] = total.astype(BF16)
        dx_copy(b, s).start()

        @pl.when(b < nb - 2)
        def _():
            start(wx_copies(b + 2, s))

        return 0

    lax.fori_loop(0, nb, dx_block, 0)

    for b in (nb - 2, nb - 1):
        dx_copy(b, b % 2).wait()
    x_out_copy(nb - 1, (nb - 1) % 2).wait()
    wait(dcat_copies())

    def drain(b, _):
        far("x", b)
        sent("x", b)
        sent("d", b)
        return 0

    lax.fori_loop(0, nb, drain, 0)


def fused(n, x, dy, gate, up, wg, wu, wd):
    own, depth = x.shape
    rows, ff = gate.shape
    nb, nf, rem = depth // BLK, ff // BLK, ff % BLK
    np1, np2 = nf + 1, 2 * nf + 2
    dma = pltpu.SemaphoreType.DMA
    hbm = pl.BlockSpec(memory_space=pl.ANY)
    flops = 2 * rows * depth * ff * 4
    return pl.pallas_call(
        functools.partial(fused_kernel, n),
        out_shape=[
            jax.ShapeDtypeStruct((ff, depth), BF16),
            jax.ShapeDtypeStruct((np2, rows, BLK), BF16),
            jax.ShapeDtypeStruct((rows, depth), BF16),
            jax.ShapeDtypeStruct((rows, depth), BF16),
        ],
        in_specs=[hbm] * 7,
        out_specs=[hbm] * 4,
        scratch_shapes=[
            pltpu.VMEM((nb, rows, BLK), BF16),
            pltpu.VMEM((np2, rows, BLK), BF16),
            pltpu.VMEM((np1, rows, BLK), F32),
            pltpu.VMEM((np1, BLK, rows), BF16),
            pltpu.VMEM((2, np2, BLK, BLK), BF16),
            pltpu.VMEM((4, rows, BLK), BF16),
            dma((nb, 4)), dma((nb, 4)), dma((nb,)), dma((nb, 4)), dma((nb, 4)), dma((2,)), dma((2,)),
            dma((2, np2)), dma((2,)), dma((2, np1)), dma((2, LATE)), dma((2, 2)), dma((2,)), dma((np2,)),
        ],
        compiler_params=pltpu.CompilerParams(collective_id=0, has_side_effects=True, vmem_limit_bytes=VMEM_LIMIT),
        cost_estimate=pl.CostEstimate(flops=flops, bytes_accessed=5 * ff * depth * 2, transcendentals=0),
        name="fused",
    )(x, dy, gate, up, wg, wu, wd)


def weights_kernel(x_ref, dcat_ref, dwd_ref, og, ou, od):
    ff = og.shape[1]
    nf, rem = ff // BLK, ff % BLK
    side = BLK - rem
    e = nf * BLK
    xt = x_ref[...].T
    for p in range(nf):
        og[:, p * BLK : (p + 1) * BLK] = dot(xt, dcat_ref[p], NN).astype(BF16)
        ou[:, p * BLK : (p + 1) * BLK] = dot(xt, dcat_ref[nf + p], NN).astype(BF16)
    both = dot(xt, dcat_ref[2 * nf], NN).astype(BF16)
    og[:, e:] = both[:, :rem]
    ou[:, e : e + side] = both[:, rem:]
    ou[:, e + side :] = dot(xt, dcat_ref[2 * nf + 1, :, : rem - side], NN).astype(BF16)
    od[...] = dwd_ref[...]


def weights(xg, dcat, dwd):
    rows, depth = xg.shape
    ff = dwd.shape[0]
    nb = depth // BLK
    return pl.pallas_call(
        weights_kernel,
        grid=(nb,),
        in_specs=[
            pl.BlockSpec((rows, BLK), lambda i: (0, i)),
            pl.BlockSpec(dcat.shape, lambda i: (0, 0, 0), pipeline_mode=pl.Buffered(1)),
            pl.BlockSpec((ff, BLK), lambda i: (0, i)),
        ],
        out_specs=[
            pl.BlockSpec((BLK, ff), lambda i: (i, 0)),
            pl.BlockSpec((BLK, ff), lambda i: (i, 0)),
            pl.BlockSpec((ff, BLK), lambda i: (0, i)),
        ],
        out_shape=[
            jax.ShapeDtypeStruct((depth, ff), BF16),
            jax.ShapeDtypeStruct((depth, ff), BF16),
            jax.ShapeDtypeStruct((ff, depth), BF16),
        ],
        compiler_params=pltpu.CompilerParams(vmem_limit_bytes=VMEM_LIMIT),
        cost_estimate=pl.CostEstimate(flops=2 * rows * depth * ff * 2, bytes_accessed=4 * ff * depth * 2, transcendentals=0),
        name="weights",
    )(xg, dcat, dwd)


def solution(mesh):
    n = mesh.shape["tp"]

    def step(x, dy, gate, up, wg, wu, wd):
        dwd, dcat, dxp, xg = fused(n, x, dy, gate, up, wg, wu, wd)
        dx = lax.psum_scatter(dxp, "tp", scatter_dimension=0, tiled=True)
        dwg, dwu, dwd = weights(xg, dcat, dwd)
        return dx, dwg, dwu, dwd

    tokens, inner, both = P(("dp", "tp"), None), P("dp", "tp"), P(None, "tp")
    return jax.shard_map(
        step,
        mesh=mesh,
        in_specs=(tokens, tokens, inner, inner, both, both, P("tp", None)),
        out_specs=(tokens, inner, inner, tokens),
        check_vma=False,
    )
```

```python
import functools

import jax
import jax.numpy as jnp
from jax import lax
from jax.experimental import pallas as pl
from jax.experimental.pallas import tpu as pltpu
from jax.sharding import PartitionSpec as P

MESH = pl.DeviceIdType.MESH
BF16, F32 = jnp.bfloat16, jnp.float32
BLK = 512
LATE = 4
ROWS = 16
VMEM_LIMIT = 66_500_000

NT = (((1,), (1,)), ((), ()))
NN = (((1,), (0,)), ((), ()))


def dot(a, b, dims):
    return lax.dot_general(a, b, dims, preferred_element_type=F32)


def act_parts(gate, up):
    g, u = gate.astype(F32), up.astype(F32)
    s = 1.0 / (1.0 + jnp.exp(-g))
    return g, u, s


def fused_kernel(
    n, x_own, dy_own, gate, up, wg, wu, wd,
    dwd, dcat_out, dxp, xg,
    dyg, dcat, acc, hid, wb, gu,
    d_send, d_recv, d_own, x_send, x_recv, x_in, x_out, w_sem, w_last, o_sem, l_sem, gu_sem, dx_sem, dc_sem,
):
    own, depth = dy_own.shape
    rows, ff = gate.shape
    nb = depth // BLK
    nf, rem = ff // BLK, ff % BLK
    half = own // 2
    side = BLK - rem
    tail = rem - side
    np1 = nf + 1
    me = lax.axis_index("tp")
    right, left = lax.rem(me + 1, n), lax.rem(me + n - 1, n)

    def cols(b):
        return pl.ds(pl.multiple_of(b * BLK, BLK), BLK)

    def own_rows(i):
        return pl.ds(pl.multiple_of(i * own, 16), own)

    def half_rows(i, second):
        return pl.ds(pl.multiple_of(i * own + second * half, 16), half)

    def remote(src, dst, send, recv, to):
        return pltpu.make_async_remote_copy(
            src_ref=src, dst_ref=dst, send_sem=send, recv_sem=recv, device_id={"tp": to}, device_id_type=MESH
        )

    def view(which, b, r):
        return dyg.at[b, r] if which == "d" else xg.at[r, cols(b)]

    def sems(which):
        return (d_send, d_recv) if which == "d" else (x_send, x_recv)

    def hop_copy(which, b, i):
        src = (dy_own if which == "d" else x_own).at[:, cols(b)]
        send, recv = sems(which)
        return remote(src, view(which, b, own_rows(me)), send.at[b, i], recv.at[b, i], (right, left)[i])

    def fwd_copy(which, b, i):
        r = half_rows((left, right)[i], i)
        send, recv = sems(which)
        return remote(view(which, b, r), view(which, b, r), send.at[b, 2 + i], recv.at[b, 2 + i], (right, left)[i])

    def hop(which, b):
        for i in (0, 1):
            hop_copy(which, b, i).start()

    def fwd(which, b):
        for i in (0, 1):
            r = own_rows((left, right)[i])
            send, recv = sems(which)
            remote(view(which, b, r), view(which, b, r), send.at[b, i], recv.at[b, i], right).wait_recv()
            fwd_copy(which, b, i).start()

    def far(which, b):
        opposite = lax.rem(me + 2, n)
        send, recv = sems(which)
        for i in (0, 1):
            r = half_rows(opposite, i)
            remote(view(which, b, r), view(which, b, r), send.at[b, 2 + i], recv.at[b, 2 + i], right).wait_recv()

    def sent(which, b):
        for i in (0, 1):
            hop_copy(which, b, i).wait_send()
            fwd_copy(which, b, i).wait_send()

    def own_copy(b):
        return pltpu.make_async_copy(dy_own.at[:, cols(b)], dyg.at[b, own_rows(me)], d_own.at[b])

    def size(p):
        return BLK if p < nf else rem

    def wd_copies(b, s):
        return [
            pltpu.make_async_copy(
                wd.at[pl.ds(p * BLK, size(p)), cols(b)], wb.at[s, p, pl.ds(0, size(p))], w_sem.at[s, p]
            )
            for p in range(np1)
        ]

    def out_copies(b, s):
        return [
            pltpu.make_async_copy(
                wb.at[s, np1 + p, pl.ds(0, size(p))], dwd.at[pl.ds(p * BLK, size(p)), cols(b)], o_sem.at[s, p]
            )
            for p in range(np1)
        ]

    def wx_copies(b, s):
        r = cols(b)
        c = [
            pltpu.make_async_copy((wg, wu)[i].at[r, pl.ds(p * BLK, BLK)], wb.at[s, i * nf + p], w_sem.at[s, i * nf + p])
            for i in (0, 1)
            for p in range(nf)
        ]
        e = nf * BLK
        c.append(
            pltpu.make_async_copy(wg.at[r, pl.ds(e, rem)], wb.at[s, 2 * nf, :, pl.ds(0, rem)], w_sem.at[s, 2 * nf])
        )
        c.append(
            pltpu.make_async_copy(wu.at[r, pl.ds(e, side)], wb.at[s, 2 * nf, :, pl.ds(rem, side)], w_last.at[s])
        )
        c.append(
            pltpu.make_async_copy(
                wu.at[r, pl.ds(e + side, tail)], wb.at[s, 2 * nf + 1, :, pl.ds(0, tail)], w_sem.at[s, 2 * nf + 1]
            )
        )
        return c

    def gu_copies(p):
        c = pl.ds(pl.multiple_of(p * BLK, BLK), BLK)
        return [
            pltpu.make_async_copy(gate.at[:, c], dcat.at[p], gu_sem.at[p, 0]),
            pltpu.make_async_copy(up.at[:, c], dcat.at[nf + p], gu_sem.at[p, 1]),
        ]

    def gu_rest():
        e = nf * BLK
        return [
            pltpu.make_async_copy(gate.at[:, pl.ds(e, rem)], dcat.at[2 * nf, :, pl.ds(0, rem)], gu_sem.at[nf, 0]),
            pltpu.make_async_copy(up.at[:, pl.ds(e, side)], dcat.at[2 * nf, :, pl.ds(rem, side)], gu_sem.at[nf, 1]),
            pltpu.make_async_copy(
                up.at[:, pl.ds(e + side, tail)], dcat.at[2 * nf + 1, :, pl.ds(0, tail)], gu_sem.at[nf + 1, 0]
            ),
        ]

    def gu_slices(p, full, t, c):
        if full:
            return dcat[p, t, c], dcat[nf + p, t, c]
        g = dcat[2 * nf, t, c]
        if c.stop <= side:
            return g, dcat[2 * nf, t, rem + c.start : rem + c.stop]
        return g, dcat[2 * nf + 1, t, c.start - side : c.stop - side]

    def late_copies(p, q, width):
        r = pl.ds(pl.multiple_of(p * BLK, BLK), width)
        return [
            pltpu.make_async_copy(
                wb.at[1, np1 + LATE * q + k, pl.ds(0, width)], dwd.at[r, cols(nb - LATE + k)], l_sem.at[q, k]
            )
            for k in range(LATE)
        ]

    def start(copies):
        for c in copies:
            c.start()

    def wait(copies):
        for c in copies:
            c.wait()

    barrier = pltpu.get_barrier_semaphore()
    for to in (left, right):
        pl.semaphore_signal(barrier, inc=1, device_id={"tp": to}, device_id_type=MESH)
    for p in range(nf):
        start(gu_copies(p))
    start(gu_rest())
    pl.semaphore_wait(barrier, 2)
    for b in range(2):
        hop("d", b)
    for b in range(nb):
        own_copy(b).start()
    start(wd_copies(0, 0))
    start(wd_copies(1, 1))

    def hidden_piece(p, width):
        for r in range(0, rows, 128):
            for c in range(0, width, 128):
                g, u, sg = act_parts(*gu_slices(p, width == BLK, slice(r, r + 128), slice(c, c + 128)))
                hid[p, c : c + 128, r : r + 128] = (g * sg * u).astype(BF16).T
        acc[p, :, :width] = jnp.zeros((rows, width), F32)

    def hidden_full(p, _):
        wait(gu_copies(p))
        hidden_piece(p, BLK)
        return 0

    lax.fori_loop(0, nf - 2, hidden_full, 0)
    fwd("d", 0)
    hop("d", 2)
    lax.fori_loop(nf - 2, nf, hidden_full, 0)
    wait(gu_rest())
    hidden_piece(nf, rem)
    dcat[2 * nf + 1, :, tail:] = jnp.zeros((rows, BLK - tail), BF16)

    def d_hidden(b, s):
        dyb = dyg[b]
        for p in range(np1):
            w = size(p)
            acc[p, :, :w] += dot(dyb, wb[s, p, :w, :], NT)

    def pass_on(b):
        @pl.when(b <= 3)
        def _():
            fwd("d", b + 1)
            hop("d", b + 3)

        @pl.when((b >= 3) & (b < nb - 2))
        def _():
            fwd("d", b + 2)

        @pl.when((b >= 3) & (b < nb - 4))
        def _():
            hop("d", b + 4)

    def both(b, _):
        s = lax.rem(b, 2)
        pass_on(b)

        wait(wd_copies(b, s))
        own_copy(b).wait()
        far("d", b)

        @pl.when(b >= 2)
        def _():
            wait(out_copies(b - 2, s))

        d_hidden(b, s)
        dyb = dyg[b]
        for p in range(np1):
            w = size(p)
            wb[s, np1 + p, :w, :] = dot(hid[p, :w, :], dyb, NN).astype(BF16)
        start(out_copies(b, s))
        start(wd_copies(b + 2, s))
        return 0

    lax.fori_loop(0, nb - LATE, both, 0)

    def only_hidden(b, _):
        s = lax.rem(b, 2)

        pass_on(b)
        wait(wd_copies(b, s))
        own_copy(b).wait()
        far("d", b)
        d_hidden(b, s)

        @pl.when(b < nb - 2)
        def _():
            start(wd_copies(b + 2, s))

        return 0

    lax.fori_loop(nb - LATE, nb, only_hidden, 0)
    for b in (nb - LATE - 2, nb - LATE - 1):
        wait(out_copies(b, b % 2))
    start(wx_copies(0, 0))
    for b in range(3):
        hop("x", b)

    def dx_copy(b, s):
        return pltpu.make_async_copy(gu.at[s], dxp.at[:, cols(b)], dx_sem.at[s])

    def dcat_copy(p):
        return pltpu.make_async_copy(dcat.at[p], dcat_out.at[p], dc_sem.at[p])

    def x_in_copy(b, s):
        return pltpu.make_async_copy(x_own.at[:, cols(b)], gu.at[2 + s, pl.ds(0, own)], x_in.at[s])

    def x_out_copy(b, s):
        return pltpu.make_async_copy(gu.at[2 + s, pl.ds(0, own)], xg.at[own_rows(me), cols(b)], x_out.at[s])

    def act_rows(p, width, t):
        if width == BLK:
            g, u, sg = act_parts(dcat[p, t, :], dcat[nf + p, t, :])
        else:
            up_rest = jnp.concatenate([dcat[2 * nf, t, rem:], dcat[2 * nf + 1, t, :tail]], axis=1)
            g, u, sg = act_parts(dcat[2 * nf, t, :rem], up_rest)
        dh = acc[p, t, :width]
        silu = g * sg
        d_up = (dh * silu).astype(BF16)
        d_gate = (dh * u * (sg + silu * (1.0 - sg))).astype(BF16)
        if width == BLK:
            dcat[p, t, :] = d_gate
            dcat[nf + p, t, :] = d_up
        else:
            dcat[2 * nf, t, :rem] = d_gate
            dcat[2 * nf, t, rem:] = d_up[:, :side]
            dcat[2 * nf + 1, t, :tail] = d_up[:, side:]

    def act_piece(p, s, width):
        steps = rows // ROWS
        for k in range(LATE):
            for r in range(k * steps // LATE, (k + 1) * steps // LATE):
                act_rows(p, width, slice(r * ROWS, (r + 1) * ROWS))
            wb[1, np1 + LATE * s + k, :width, :] = dot(hid[p, :width, :], dyg[nb - LATE + k], NN).astype(BF16)
        start(late_copies(p, s, width))

    def act_full(p, _):
        s = lax.rem(p, 2)

        @pl.when(p >= 2)
        def _():
            wait(late_copies(p - 2, s, BLK))

        act_piece(p, s, BLK)
        return 0

    lax.fori_loop(0, nf, act_full, 0)
    wait(late_copies(nf - 2, nf % 2, BLK))
    act_piece(nf, nf % 2, rem)
    x_in_copy(0, 0).start()
    wait(late_copies(nf - 1, (nf - 1) % 2, BLK))
    wait(late_copies(nf, nf % 2, rem))
    start(wx_copies(1, 1))

    def dx_block(b, _):
        s = lax.rem(b, 2)
        fwd("x", b)

        @pl.when(b < nb - 3)
        def _():
            hop("x", b + 3)

        x_in_copy(b, s).wait()
        x_out_copy(b, s).start()

        @pl.when(b >= 1)
        def _():
            x_out_copy(b - 1, 1 - s).wait()

        @pl.when(b < nb - 1)
        def _():
            x_in_copy(b + 1, 1 - s).start()

        @pl.when(b >= 2)
        def _():
            dx_copy(b - 2, s).wait()

        for p in (2 * b, 2 * b + 1):

            @pl.when(p < 2 * nf + 2)
            def _():
                dcat_copy(p).start()

        wait(wx_copies(b, s))
        total = dot(dcat[0], wb[s, 0], NT)
        for p in range(1, 2 * nf + 1):
            total += dot(dcat[p], wb[s, p], NT)
        total += dot(dcat[2 * nf + 1, :, :tail], wb[s, 2 * nf + 1, :, :tail], NT)
        gu[s] = total.astype(BF16)
        dx_copy(b, s).start()

        @pl.when(b < nb - 2)
        def _():
            start(wx_copies(b + 2, s))

        return 0

    lax.fori_loop(0, nb, dx_block, 0)

    for b in (nb - 2, nb - 1):
        dx_copy(b, b % 2).wait()
    x_out_copy(nb - 1, (nb - 1) % 2).wait()

    for p in range(2 * nf + 2):
        dcat_copy(p).wait()

    def drain(b, _):
        far("x", b)
        sent("x", b)
        sent("d", b)
        return 0

    lax.fori_loop(0, nb, drain, 0)


def fused(n, x, dy, gate, up, wg, wu, wd):
    own, depth = x.shape
    rows, ff = gate.shape
    nb, nf, rem = depth // BLK, ff // BLK, ff % BLK
    np1, np2 = nf + 1, 2 * nf + 2
    dma = pltpu.SemaphoreType.DMA
    hbm = pl.BlockSpec(memory_space=pl.ANY)
    flops = 2 * rows * depth * ff * 4
    return pl.pallas_call(
        functools.partial(fused_kernel, n),
        out_shape=[
            jax.ShapeDtypeStruct((ff, depth), BF16),
            jax.ShapeDtypeStruct((np2, rows, BLK), BF16),
            jax.ShapeDtypeStruct((rows, depth), BF16),
            jax.ShapeDtypeStruct((rows, depth), BF16),
        ],
        in_specs=[hbm] * 7,
        out_specs=[hbm] * 4,
        scratch_shapes=[
            pltpu.VMEM((nb, rows, BLK), BF16),
            pltpu.VMEM((np2, rows, BLK), BF16),
            pltpu.VMEM((np1, rows, BLK), F32),
            pltpu.VMEM((np1, BLK, rows), BF16),
            pltpu.VMEM((2, np2, BLK, BLK), BF16),
            pltpu.VMEM((4, rows, BLK), BF16),
            dma((nb, 4)), dma((nb, 4)), dma((nb,)), dma((nb, 4)), dma((nb, 4)), dma((2,)), dma((2,)),
            dma((2, np2)), dma((2,)), dma((2, np1)), dma((2, LATE)), dma((nf + 2, 2)), dma((2,)), dma((np2,)),
        ],
        compiler_params=pltpu.CompilerParams(
            collective_id=0, has_side_effects=True, vmem_limit_bytes=VMEM_LIMIT,
        ),
        cost_estimate=pl.CostEstimate(flops=flops, bytes_accessed=5 * ff * depth * 2, transcendentals=0),
        name="fused",
    )(x, dy, gate, up, wg, wu, wd)


def weights_kernel(xg, dcat_in, dwd, og, ou, od, dcat, xb, gb, ub, tb, d_sem, x_sem, g_sem, u_sem, i_sem, t_sem):
    depth, ff = og.shape
    nb, nf, rem = depth // BLK, ff // BLK, ff % BLK
    side, e = BLK - rem, nf * BLK
    chunk = tb.shape[1]
    chunks, group = ff // chunk, tb.shape[0] // 2

    def cols(i):
        return pl.ds(pl.multiple_of(i * BLK, BLK), BLK)

    def x_copy(i, s):
        return pltpu.make_async_copy(xg.at[:, cols(i)], xb.at[s], x_sem.at[s])

    def out_copies(i, s):
        return (
            pltpu.make_async_copy(gb.at[s], og.at[cols(i)], g_sem.at[s]),
            pltpu.make_async_copy(ub.at[s], ou.at[cols(i)], u_sem.at[s]),
        )

    def through(step, s, f):
        for k in range(group):
            j = step * group + k
            r = pl.ds(pl.multiple_of(j * chunk, chunk), chunk)
            t = s * group + k

            @pl.when(j < chunks)
            def _():
                f(
                    lambda: pltpu.make_async_copy(dwd.at[r], tb.at[t], i_sem.at[t]),
                    lambda: pltpu.make_async_copy(tb.at[t], od.at[r], t_sem.at[t]),
                )

    def read(i, o):
        i().start()

    def write(i, o):
        i().wait()
        o().start()

    def done(i, o):
        o().wait()

    load = pltpu.make_async_copy(dcat_in, dcat, d_sem)
    x_copy(0, 0).start()
    load.start()
    x_copy(1, 1).start()
    through(0, 0, read)
    load.wait()

    def body(i, _):
        s = lax.rem(i, 2)
        x_copy(i, s).wait()
        through(i, s, write)

        @pl.when(i >= 1)
        def _():
            through(i - 1, 1 - s, done)

        through(i + 1, 1 - s, read)

        @pl.when(i >= 2)
        def _():
            for c in out_copies(i - 2, s):
                c.wait()

        xt = xb[s].T
        for p in range(nf):
            gb[s, :, p * BLK : (p + 1) * BLK] = dot(xt, dcat[p], NN).astype(BF16)
            ub[s, :, p * BLK : (p + 1) * BLK] = dot(xt, dcat[nf + p], NN).astype(BF16)
        both = dot(xt, dcat[2 * nf], NN).astype(BF16)
        gb[s, :, e:] = both[:, :rem]
        ub[s, :, e : e + side] = both[:, rem:]
        ub[s, :, e + side :] = dot(xt, dcat[2 * nf + 1, :, : rem - side], NN).astype(BF16)
        for c in out_copies(i, s):
            c.start()

        @pl.when(i < nb - 2)
        def _():
            x_copy(i + 2, s).start()

        return 0

    lax.fori_loop(0, nb, body, 0)
    through(nb - 1, (nb - 1) % 2, done)
    for i in (nb - 2, nb - 1):
        for c in out_copies(i, i % 2):
            c.wait()


def weights(xg, dcat, dwd):
    rows, depth = xg.shape
    ff = dwd.shape[0]
    chunk, group = 128, 3
    dma = pltpu.SemaphoreType.DMA
    hbm = pl.BlockSpec(memory_space=pl.ANY)
    return pl.pallas_call(
        weights_kernel,
        in_specs=[hbm] * 3,
        out_specs=[hbm] * 3,
        out_shape=[
            jax.ShapeDtypeStruct((depth, ff), BF16),
            jax.ShapeDtypeStruct((depth, ff), BF16),
            jax.ShapeDtypeStruct((ff, depth), BF16),
        ],
        scratch_shapes=[
            pltpu.VMEM(dcat.shape, BF16),
            pltpu.VMEM((2, rows, BLK), BF16),
            pltpu.VMEM((2, BLK, ff), BF16),
            pltpu.VMEM((2, BLK, ff), BF16),
            pltpu.VMEM((2 * group, chunk, depth), BF16),
            dma, dma((2,)), dma((2,)), dma((2,)), dma((2 * group,)), dma((2 * group,)),
        ],
        compiler_params=pltpu.CompilerParams(vmem_limit_bytes=VMEM_LIMIT),
        cost_estimate=pl.CostEstimate(flops=2 * rows * depth * ff * 2, bytes_accessed=4 * ff * depth * 2, transcendentals=0),
        name="weights",
    )(xg, dcat, dwd)


def solution(mesh):
    n = mesh.shape["tp"]

    def step(x, dy, gate, up, wg, wu, wd):
        dwd, dcat, dxp, xg = fused(n, x, dy, gate, up, wg, wu, wd)
        dx = lax.psum_scatter(dxp, "tp", scatter_dimension=0, tiled=True)
        dwg, dwu, dwd = weights(xg, dcat, dwd)
        return dx, dwg, dwu, dwd

    tokens, inner, both = P(("dp", "tp"), None), P("dp", "tp"), P(None, "tp")
    return jax.shard_map(
        step,
        mesh=mesh,
        in_specs=(tokens, tokens, inner, inner, both, both, P("tp", None)),
        out_specs=(tokens, inner, inner, tokens),
        check_vma=False,
    )
```

```python
import functools

import jax
import jax.numpy as jnp
from jax import lax
from jax.experimental import pallas as pl
from jax.experimental.pallas import tpu as pltpu
from jax.sharding import PartitionSpec as P

MESH = pl.DeviceIdType.MESH
BF16, F32 = jnp.bfloat16, jnp.float32
BLK = 512
LATE = 4
ROWS = 16
VMEM_LIMIT = 66_500_000

NT = (((1,), (1,)), ((), ()))
NN = (((1,), (0,)), ((), ()))


def dot(a, b, dims):
    return lax.dot_general(a, b, dims, preferred_element_type=F32)


def act_parts(gate, up):
    g, u = gate.astype(F32), up.astype(F32)
    s = 1.0 / (1.0 + jnp.exp(-g))
    return g, u, s


def fused_kernel(
    n, x_own, dy_own, gate, up, wg, wu, wd,
    dwd, dcat_out, dxp, xg,
    dyg, dcat, acc, hid, wb, gu,
    d_send, d_recv, d_own, x_send, x_recv, x_in, x_out, w_sem, o_sem, l_sem, gu_sem, dx_sem, dc_sem,
):
    own, depth = dy_own.shape
    rows, ff = gate.shape
    nb = depth // BLK
    nf, rem = ff // BLK, ff % BLK
    half = own // 2
    side = BLK - rem
    tail = rem - side
    np1 = nf + 1
    early = nb - LATE
    me = lax.axis_index("tp")
    right, left, opposite = lax.rem(me + 1, n), lax.rem(me + n - 1, n), lax.rem(me + 2, n)

    def cols(b):
        return pl.ds(pl.multiple_of(b * BLK, BLK), BLK)

    def own_rows(i):
        return pl.ds(pl.multiple_of(i * own, 16), own)

    def half_rows(i, second):
        return pl.ds(pl.multiple_of(i * own + second * half, 16), half)

    def remote(src, dst, send, recv, to):
        return pltpu.make_async_remote_copy(
            src_ref=src, dst_ref=dst, send_sem=send, recv_sem=recv, device_id={"tp": to}, device_id_type=MESH
        )

    def view(which, b, r):
        return dyg.at[b, r] if which == "d" else xg.at[r, cols(b)]

    def sems(which):
        return (d_send, d_recv) if which == "d" else (x_send, x_recv)

    def hop(which, b):
        send, recv = sems(which)
        src = (dy_own if which == "d" else x_own).at[:, cols(b)]
        for i, to in enumerate((right, left)):
            remote(src, view(which, b, own_rows(me)), send, recv.at[b, i], to).start()

    def fwd(which, b):
        send, recv = sems(which)
        for i, (source, to) in enumerate(((left, right), (right, left))):
            v = view(which, b, own_rows(source))
            remote(v, v, send, recv.at[b, i], to).wait_recv()
            v = view(which, b, half_rows(source, i))
            remote(v, v, send, recv.at[b, 2], to).start()

    def far(which, b):
        send, recv = sems(which)
        v = view(which, b, own_rows(opposite))
        remote(v, v, send, recv.at[b, 2], right).wait_recv()

    def sent(which):
        v = dyg.at[:, pl.ds(0, 3 * own)]
        remote(v, v, sems(which)[0], sems(which)[1].at[0, 0], right).wait_send()

    def own_copies():
        return [pltpu.make_async_copy(dy_own.at[:, cols(b)], dyg.at[b, own_rows(me)], d_own) for b in range(nb)]

    def own_wait():
        v = dyg.at[:, own_rows(me)]
        pltpu.make_async_copy(v, v, d_own).wait()

    def size(p):
        return BLK if p < nf else rem

    def wd_copies(b, s):
        return [
            pltpu.make_async_copy(
                wd.at[pl.ds(p * BLK, size(p)), cols(b)], wb.at[s, p, pl.ds(0, size(p))], w_sem.at[s, p // nf]
            )
            for p in range(np1)
        ]

    def wait_pieces(sem, s, first, count, rest):
        v = wb.at[s, pl.ds(first, count)]
        pltpu.make_async_copy(v, v, sem.at[s, 0]).wait()
        v = wb.at[s, first + count, *rest]
        pltpu.make_async_copy(v, v, sem.at[s, 1]).wait()

    def wd_wait(s):
        wait_pieces(w_sem, s, 0, nf, (pl.ds(0, rem),))

    def out_copies(b, s):
        return [
            pltpu.make_async_copy(
                wb.at[s, np1 + p, pl.ds(0, size(p))], dwd.at[pl.ds(p * BLK, size(p)), cols(b)], o_sem.at[s, p // nf]
            )
            for p in range(np1)
        ]

    def out_wait(s):
        wait_pieces(o_sem, s, np1, nf, (pl.ds(0, rem),))

    def wx_copies(b, s):
        r, e = cols(b), nf * BLK
        c = [
            pltpu.make_async_copy((wg, wu)[i].at[r, pl.ds(p * BLK, BLK)], wb.at[s, i * nf + p], w_sem.at[s, 0])
            for i in (0, 1)
            for p in range(nf)
        ]
        mixed = wb.at[s, 2 * nf]
        c.append(pltpu.make_async_copy(wg.at[r, pl.ds(e, rem)], mixed.at[:, pl.ds(0, rem)], w_sem.at[s, 0]))
        c.append(pltpu.make_async_copy(wu.at[r, pl.ds(e, side)], mixed.at[:, pl.ds(rem, side)], w_sem.at[s, 0]))
        last = wb.at[s, 2 * nf + 1, :, pl.ds(0, tail)]
        c.append(pltpu.make_async_copy(wu.at[r, pl.ds(e + side, tail)], last, w_sem.at[s, 1]))
        return c

    def wx_wait(s):
        wait_pieces(w_sem, s, 0, 2 * nf + 1, (slice(None), pl.ds(0, tail)))

    def gu_copies(p):
        c = pl.ds(pl.multiple_of(p * BLK, BLK), BLK)
        return [
            pltpu.make_async_copy(gate.at[:, c], dcat.at[p], gu_sem.at[p]),
            pltpu.make_async_copy(up.at[:, c], dcat.at[nf + p], gu_sem.at[p]),
        ]

    def gu_wait(p):
        v = dcat.at[pl.ds(0, 2)]
        pltpu.make_async_copy(v, v, gu_sem.at[p]).wait()

    def gu_rest():
        e = nf * BLK
        mixed, last = dcat.at[2 * nf], dcat.at[2 * nf + 1, :, pl.ds(0, tail)]
        return [
            pltpu.make_async_copy(gate.at[:, pl.ds(e, rem)], mixed.at[:, pl.ds(0, rem)], gu_sem.at[nf]),
            pltpu.make_async_copy(up.at[:, pl.ds(e, side)], mixed.at[:, pl.ds(rem, side)], gu_sem.at[nf]),
            pltpu.make_async_copy(up.at[:, pl.ds(e + side, tail)], last, gu_sem.at[nf + 1]),
        ]

    def gu_rest_wait():
        v = dcat.at[2 * nf]
        pltpu.make_async_copy(v, v, gu_sem.at[nf]).wait()
        v = dcat.at[2 * nf + 1, :, pl.ds(0, tail)]
        pltpu.make_async_copy(v, v, gu_sem.at[nf + 1]).wait()

    def gu_slices(p, full, t, c):
        if full:
            return dcat[p, t, c], dcat[nf + p, t, c]
        g = dcat[2 * nf, t, c]
        if c.stop <= side:
            return g, dcat[2 * nf, t, rem + c.start : rem + c.stop]
        return g, dcat[2 * nf + 1, t, c.start - side : c.stop - side]

    def late_copies(p, q, width):
        r = pl.ds(pl.multiple_of(p * BLK, BLK), width)
        return [
            pltpu.make_async_copy(
                wb.at[1, np1 + LATE * q + k, pl.ds(0, width)], dwd.at[r, cols(nb - LATE + k)], l_sem.at[q]
            )
            for k in range(LATE)
        ]

    def late_wait(q, width):
        v = wb.at[1, pl.ds(np1 + LATE * q, LATE), pl.ds(0, width)]
        pltpu.make_async_copy(v, v, l_sem.at[q]).wait()

    def start(copies):
        for c in copies:
            c.start()

    barrier = pltpu.get_barrier_semaphore()
    for to in (left, right):
        pl.semaphore_signal(barrier, inc=1, device_id={"tp": to}, device_id_type=MESH)
    for p in range(3):
        start(gu_copies(p))
    start(wd_copies(nb - 1, 0))
    start(own_copies())
    for p in range(3, nf):
        start(gu_copies(p))
    start(gu_rest())
    start(wd_copies(nb - 2, 1))

    def clear(p, _):
        acc[p] = jnp.zeros((rows, BLK), F32)
        return 0

    lax.fori_loop(0, np1, clear, 0)
    dcat[2 * nf + 1, :, tail:] = jnp.zeros((rows, BLK - tail), BF16)

    def hidden_piece(p, width):
        for r in range(0, rows, 128):
            for c in range(0, width, 128):
                g, u, sg = act_parts(*gu_slices(p, width == BLK, slice(r, r + 128), slice(c, c + 128)))
                hid[p, c : c + 128, r : r + 128] = (g * sg * u).astype(BF16).T

    def d_hidden(b, s, devices):
        dyb = jnp.concatenate([dyg[b, own_rows(d)] for d in devices], axis=0)
        for p in range(np1):
            w = size(p)
            terms = dot(dyb, wb[s, p, :w, :], NT)
            for k, d in enumerate(devices):
                acc[p, own_rows(d), :w] += terms[k * own : (k + 1) * own]

    def hidden_full(p, _):
        gu_wait(p)
        hidden_piece(p, BLK)
        return 0

    def hidden_and_own(p, _):
        k = p - alone
        s = lax.rem(k, 2)

        @pl.when(p == nf - 2)
        def _():
            fwd("d", 0)
            hop("d", 2)

        gu_wait(p)
        wd_wait(s)
        hidden_piece(p, BLK)
        d_hidden(nb - 1 - k, s, (me,))
        start(wd_copies(jnp.where(k < LATE - 2, nb - 3 - k, k - LATE + 2), s))
        return 0

    alone = np1 - LATE
    lax.fori_loop(0, 2, hidden_full, 0)
    pl.semaphore_wait(barrier, 2)
    for b in range(2):
        hop("d", b)
    lax.fori_loop(2, alone, hidden_full, 0)
    own_wait()
    lax.fori_loop(alone, nf, hidden_and_own, 0)
    gu_rest_wait()
    s = (LATE - 1) % 2
    wd_wait(s)
    hidden_piece(nf, rem)
    d_hidden(nb - LATE, s, (me,))
    start(wd_copies(1, s))

    def pass_on(b):
        @pl.when(b <= 3)
        def _():
            fwd("d", b + 1)
            hop("d", b + 3)

        @pl.when((b >= 3) & (b < nb - 2))
        def _():
            fwd("d", b + 2)

        @pl.when((b >= 3) & (b < nb - 4))
        def _():
            hop("d", b + 4)

    def both(b, _):
        s = lax.rem(b, 2)
        pass_on(b)

        far("d", b)

        wd_wait(s)

        @pl.when(b >= 2)
        def _():
            out_wait(s)

        d_hidden(b, s, range(n))
        dyb = dyg[b]
        for p in range(np1):
            w = size(p)
            wb[s, np1 + p, :w, :] = dot(hid[p, :w, :], dyb, NN).astype(BF16)
        start(out_copies(b, s))
        start(wd_copies(b + 2, s))
        return 0

    lax.fori_loop(0, early, both, 0)

    def only_hidden(b, _):
        s = lax.rem(b, 2)

        pass_on(b)
        wd_wait(s)
        far("d", b)
        d_hidden(b, s, (right, opposite, left))

        @pl.when(b < nb - 2)
        def _():
            start(wd_copies(b + 2, s))

        return 0

    lax.fori_loop(early, nb, only_hidden, 0)
    for s in (0, 1):
        out_wait(s)
    start(wx_copies(0, 0))
    for b in range(3):
        hop("x", b)

    def dx_copy(b, s):
        return pltpu.make_async_copy(gu.at[s], dxp.at[:, cols(b)], dx_sem.at[s])

    def dcat_copy(p):
        return pltpu.make_async_copy(dcat.at[p], dcat_out.at[p], dc_sem)

    def x_in_copy(b, s):
        return pltpu.make_async_copy(x_own.at[:, cols(b)], gu.at[2 + s, pl.ds(0, own)], x_in.at[s])

    def x_out_copy(b, s):
        return pltpu.make_async_copy(gu.at[2 + s, pl.ds(0, own)], xg.at[own_rows(me), cols(b)], x_out.at[s])

    def act_rows(p, width, t):
        if width == BLK:
            g, u, sg = act_parts(dcat[p, t, :], dcat[nf + p, t, :])
        else:
            up_rest = jnp.concatenate([dcat[2 * nf, t, rem:], dcat[2 * nf + 1, t, :tail]], axis=1)
            g, u, sg = act_parts(dcat[2 * nf, t, :rem], up_rest)
        dh = acc[p, t, :width]
        silu = g * sg
        d_up = (dh * silu).astype(BF16)
        d_gate = (dh * u * (sg + silu * (1.0 - sg))).astype(BF16)
        if width == BLK:
            dcat[p, t, :] = d_gate
            dcat[nf + p, t, :] = d_up
        else:
            dcat[2 * nf, t, :rem] = d_gate
            dcat[2 * nf, t, rem:] = d_up[:, :side]
            dcat[2 * nf + 1, t, :tail] = d_up[:, side:]

    def act_piece(p, s, width):
        steps = rows // ROWS
        for k in range(LATE):
            for r in range(k * steps // LATE, (k + 1) * steps // LATE):
                act_rows(p, width, slice(r * ROWS, (r + 1) * ROWS))
            wb[1, np1 + LATE * s + k, :width, :] = dot(hid[p, :width, :], dyg[nb - LATE + k], NN).astype(BF16)
        start(late_copies(p, s, width))

    def act_full(p, _):
        s = lax.rem(p, 2)

        @pl.when(p >= 2)
        def _():
            late_wait(s, BLK)

        act_piece(p, s, BLK)
        return 0

    lax.fori_loop(0, nf, act_full, 0)
    late_wait(nf % 2, BLK)
    act_piece(nf, nf % 2, rem)
    x_in_copy(0, 0).start()
    late_wait((nf - 1) % 2, BLK)
    late_wait(nf % 2, rem)
    start(wx_copies(1, 1))

    def dx_block(b, _):
        s = lax.rem(b, 2)
        fwd("x", b)

        @pl.when(b < nb - 3)
        def _():
            hop("x", b + 3)

        x_in_copy(b, s).wait()
        x_out_copy(b, s).start()

        @pl.when(b >= 1)
        def _():
            x_out_copy(b - 1, 1 - s).wait()

        @pl.when(b < nb - 1)
        def _():
            x_in_copy(b + 1, 1 - s).start()

        @pl.when(b >= 2)
        def _():
            dx_copy(b - 2, s).wait()

        for p in (2 * b, 2 * b + 1):

            @pl.when(p < 2 * nf + 2)
            def _():
                dcat_copy(p).start()

        wx_wait(s)
        total = dot(dcat[0], wb[s, 0], NT)
        for p in range(1, 2 * nf + 1):
            total += dot(dcat[p], wb[s, p], NT)
        total += dot(dcat[2 * nf + 1, :, :tail], wb[s, 2 * nf + 1, :, :tail], NT)
        gu[s] = total.astype(BF16)
        dx_copy(b, s).start()

        @pl.when(b < nb - 2)
        def _():
            start(wx_copies(b + 2, s))

        return 0

    lax.fori_loop(0, nb, dx_block, 0)

    for b in (nb - 2, nb - 1):
        dx_copy(b, b % 2).wait()
    x_out_copy(nb - 1, (nb - 1) % 2).wait()

    pltpu.make_async_copy(dcat, dcat_out, dc_sem).wait()
    for b in range(nb):
        far("x", b)
    sent("x")
    sent("d")


def fused(n, x, dy, gate, up, wg, wu, wd):
    own, depth = x.shape
    rows, ff = gate.shape
    nb, nf, rem = depth // BLK, ff // BLK, ff % BLK
    np1, np2 = nf + 1, 2 * nf + 2
    dma = pltpu.SemaphoreType.DMA
    hbm = pl.BlockSpec(memory_space=pl.ANY)
    flops = 2 * rows * depth * ff * 4
    return pl.pallas_call(
        functools.partial(fused_kernel, n),
        out_shape=[
            jax.ShapeDtypeStruct((ff, depth), BF16),
            jax.ShapeDtypeStruct((np2, rows, BLK), BF16),
            jax.ShapeDtypeStruct((rows, depth), BF16),
            jax.ShapeDtypeStruct((rows, depth), BF16),
        ],
        in_specs=[hbm] * 7,
        out_specs=[hbm] * 4,
        scratch_shapes=[
            pltpu.VMEM((nb, rows, BLK), BF16),
            pltpu.VMEM((np2, rows, BLK), BF16),
            pltpu.VMEM((np1, rows, BLK), F32),
            pltpu.VMEM((np1, BLK, rows), BF16),
            pltpu.VMEM((2, np2, BLK, BLK), BF16),
            pltpu.VMEM((4, rows, BLK), BF16),
            dma, dma((nb, 3)), dma, dma, dma((nb, 3)), dma((2,)), dma((2,)),
            dma((2, 2)), dma((2, 2)), dma((2,)), dma((nf + 2,)), dma((2,)), dma,
        ],
        compiler_params=pltpu.CompilerParams(
            collective_id=0, has_side_effects=True, vmem_limit_bytes=VMEM_LIMIT,
        ),
        cost_estimate=pl.CostEstimate(flops=flops, bytes_accessed=5 * ff * depth * 2, transcendentals=0),
        name="fused",
    )(x, dy, gate, up, wg, wu, wd)


def weights_kernel(xg, dcat_in, dwd, og, ou, od, dcat, xb, xt, gb, ub, tb, d_sem, x_sem, g_sem, u_sem, i_sem, t_sem):
    depth, ff = og.shape
    nb, nf, rem = depth // BLK, ff // BLK, ff % BLK
    side, e = BLK - rem, nf * BLK
    chunk = tb.shape[1]
    chunks = nb - 1
    assert chunk * chunks >= ff

    def cols(i):
        return pl.ds(pl.multiple_of(i * BLK, BLK), BLK)

    def x_copy(i, s):
        return pltpu.make_async_copy(xg.at[:, cols(i)], xb.at[s], x_sem.at[s])

    def load(p):
        for q in (p, nf + p) if p < nf else (2 * nf, 2 * nf + 1):
            pltpu.make_async_copy(dcat_in.at[q], dcat.at[q], d_sem.at[p]).start()

    def loaded(p):
        v = dcat.at[pl.ds(0, 2)]
        pltpu.make_async_copy(v, v, d_sem.at[p]).wait()

    def out_copies(i, s):
        return (
            pltpu.make_async_copy(gb.at[s], og.at[cols(i)], g_sem.at[s]),
            pltpu.make_async_copy(ub.at[s], ou.at[cols(i)], u_sem.at[s]),
        )

    def through_in(j, s):
        r = pl.ds(pl.multiple_of(jnp.minimum(j * chunk, ff - chunk), 128), chunk)
        return pltpu.make_async_copy(dwd.at[r], tb.at[s], i_sem.at[s])

    def through_out(j, s):
        r = pl.ds(pl.multiple_of(jnp.minimum(j * chunk, ff - chunk), 128), chunk)
        return pltpu.make_async_copy(tb.at[s], od.at[r], t_sem.at[s])

    def rest(s, t):
        both = dot(t, dcat[2 * nf], NN).astype(BF16)
        gb[s, :, e:] = both[:, :rem]
        ub[s, :, e : e + side] = both[:, rem:]
        ub[s, :, e + side :] = dot(t, dcat[2 * nf + 1, :, : rem - side], NN).astype(BF16)

    x_copy(0, 0).start()
    for p in range(nf + 1):
        load(p)
    x_copy(1, 1).start()
    through_in(0, 0).start()
    x_copy(0, 0).wait()
    xt[...] = xb[0].T

    def piece(p, _):
        loaded(p)
        t = xt[...]
        gb[0, :, cols(p)] = dot(t, dcat[p], NN).astype(BF16)
        ub[0, :, cols(p)] = dot(t, dcat[nf + p], NN).astype(BF16)
        return 0

    lax.fori_loop(0, nf, piece, 0)
    loaded(nf)
    rest(0, xt[...])
    for c in out_copies(0, 0):
        c.start()
    x_copy(2, 0).start()

    def body(i, _):
        s = lax.rem(i, 2)
        j = i - 1
        x_copy(i, s).wait()


        @pl.when(j >= 1)
        def _():
            through_out(j - 1, s).wait()

        through_in(j, 1 - s).wait()
        through_out(j, 1 - s).start()

        @pl.when(j + 1 < chunks)
        def _():
            through_in(j + 1, s).start()

        @pl.when(i >= 2)
        def _():
            for c in out_copies(i - 2, s):
                c.wait()

        t = xb[s].T
        for p in range(nf):
            gb[s, :, p * BLK : (p + 1) * BLK] = dot(t, dcat[p], NN).astype(BF16)
            ub[s, :, p * BLK : (p + 1) * BLK] = dot(t, dcat[nf + p], NN).astype(BF16)
        rest(s, t)
        for c in out_copies(i, s):
            c.start()

        @pl.when(i < nb - 2)
        def _():
            x_copy(i + 2, s).start()

        return 0

    lax.fori_loop(1, nb, body, 0)
    through_out(chunks - 1, (chunks - 1) % 2).wait()
    for i in (nb - 2, nb - 1):
        for c in out_copies(i, i % 2):
            c.wait()


def weights(xg, dcat, dwd):
    rows, depth = xg.shape
    ff = dwd.shape[0]
    chunk = -(-ff // (128 * (depth // BLK - 1))) * 128
    dma = pltpu.SemaphoreType.DMA
    hbm = pl.BlockSpec(memory_space=pl.ANY)
    return pl.pallas_call(
        weights_kernel,
        in_specs=[hbm] * 3,
        out_specs=[hbm] * 3,
        out_shape=[
            jax.ShapeDtypeStruct((depth, ff), BF16),
            jax.ShapeDtypeStruct((depth, ff), BF16),
            jax.ShapeDtypeStruct((ff, depth), BF16),
        ],
        scratch_shapes=[
            pltpu.VMEM(dcat.shape, BF16),
            pltpu.VMEM((2, rows, BLK), BF16),
            pltpu.VMEM((BLK, rows), BF16),
            pltpu.VMEM((2, BLK, ff), BF16),
            pltpu.VMEM((2, BLK, ff), BF16),
            pltpu.VMEM((2, chunk, depth), BF16),
            dma((ff // BLK + 1,)), dma((2,)), dma((2,)), dma((2,)), dma((2,)), dma((2,)),
        ],
        compiler_params=pltpu.CompilerParams(vmem_limit_bytes=VMEM_LIMIT),
        cost_estimate=pl.CostEstimate(flops=2 * rows * depth * ff * 2, bytes_accessed=4 * ff * depth * 2, transcendentals=0),
        name="weights",
    )(xg, dcat, dwd)


def solution(mesh):
    n = mesh.shape["tp"]

    def step(x, dy, gate, up, wg, wu, wd):
        dwd, dcat, dxp, xg = fused(n, x, dy, gate, up, wg, wu, wd)
        dx = lax.psum_scatter(dxp, "tp", scatter_dimension=0, tiled=True)
        dwg, dwu, dwd = weights(xg, dcat, dwd)
        return dx, dwg, dwu, dwd

    tokens, inner, both = P(("dp", "tp"), None), P("dp", "tp"), P(None, "tp")
    return jax.shard_map(
        step,
        mesh=mesh,
        in_specs=(tokens, tokens, inner, inner, both, both, P("tp", None)),
        out_specs=(tokens, inner, inner, tokens),
        check_vma=False,
    )
```
